32 devices in a mesh: mem: 4 (over y, x), tile: 8 (over z, core).
Axes of the slice: x: 2, y: 2, z: 4, core: 2. Of those that a mesh axis runs over, the one named last changes fastest.
Arguments:
- ensemble: float32 [1024, 3, 64, 256], P('mem', None, 'tile'), may hold values from -4.5 to 5
- obs_cells: int32 [8, 256], replicated, may hold values from 0 to 6143
- region_tile: int32 [8], replicated, may hold values from 0 to 7, each once
- obs_values: float32 [8, 256], replicated, may hold values from -5.6 to 5.6
- obs_error: float32 [8, 256], replicated, may hold values from 0.05 to 0.75
Outputs:
- analysis: float32 [1024, 3, 64, 256], P('mem', None, 'tile')
The draws below stay inside these ranges and needn't reach their ends.
Inputs may be any that keep to these rules, and one draw needn't show every extreme that they name: `obs_cells`: row r lists flat indices into the values of tile region_tile[r], ordered by field, then row within the tile, then column; indices may repeat. `region_tile`: each tile holds exactly one region.
All inputs are finite; a program needn't handle non-finite values.
Results may differ from the reference program's by a relative error of at most 0.00029.
Values sent between devices are 32-bit elements; how exact they have to be, the bound alone decides.
No kernel may reach another device: no remote copies, remote signals or barrier semaphores. Data moves between devices by JAX's collectives and lax.ppermute only.
A program may use at most 128 MiB of HBM per device.

```python
import math
import jax
import jax.numpy as jnp
from jax import lax

ENSEMBLE_SIZE = 1024
MESH_LONGITUDES = 256
BLOCK_LATITUDES = 8
OBS = 256
STEPS = 4
DEGREE = 4
GY = 64
VALS_T = 6144
REGION_TOTAL = 8
N_MEM = 4
N_TILE = 8


def draw_ensemble(key, part):
    sample = jnp.clip(jax.random.normal(key, (ENSEMBLE_SIZE, 3, GY, MESH_LONGITUDES), jnp.float32), -3.0, 3.0)
    return 0.5 * sample


def draw_obs_values(key, part):
    position = jnp.arange(REGION_TOTAL, dtype=jnp.float32) / max(REGION_TOTAL - 1, 1)
    sample = jnp.clip(jax.random.normal(key, (REGION_TOTAL, OBS), jnp.float32), -3.0, 3.0)
    return sample * jnp.sqrt(1.0 + 2.0 * position)[:, None]


def draw_obs_error(key, part):
    rising = 1.0 + 2.0 * jnp.arange(REGION_TOTAL, dtype=jnp.float32) / max(REGION_TOTAL - 1, 1)
    sample = jnp.exp(jax.random.uniform(key, (REGION_TOTAL, OBS), jnp.float32, math.log(0.05), math.log(0.25)))
    return sample * rising[:, None]


def with_ends(array, stream_key, low, top_value):
    longest = array.shape.index(max(array.shape))
    spots = []
    for shift in (0, 1):
        where = [jax.random.randint(jax.random.fold_in(stream_key, axis), (), 0, length) for axis, length in enumerate(array.shape)]
        where[longest] = (where[longest] + shift) % array.shape[longest]
        spots.append(tuple(where))
    return array.at[spots[0]].set(low).at[spots[1]].set(top_value)


def setup_inputs(seed: int = 0) -> dict:
    splits = jax.random.split(jax.random.key(seed), 6)
    return {
        "ensemble": draw_ensemble(jax.random.fold_in(splits[5], 71), 0),
        "obs_cells": with_ends(jax.random.randint(splits[1], (REGION_TOTAL, OBS), 0, VALS_T), jax.random.fold_in(splits[1], 1), 0, VALS_T - 1).astype(jnp.int32),
        "region_tile": jax.random.permutation(splits[2], N_TILE).astype(jnp.int32),
        "obs_values": draw_obs_values(jax.random.fold_in(splits[5], 71), 0),
        "obs_error": draw_obs_error(jax.random.fold_in(splits[5], 71), 0),
    }


DEPTH = 1.0
GRAVITY = 1.0
CORIOLIS = 0.5
TIMESTEP = 0.3
DIFFUSE = 0.1
PRECISE = lax.Precision.HIGHEST

def east_diff(quantity):
    return 0.5 * (jnp.roll(quantity, -1, axis=-1) - jnp.roll(quantity, 1, axis=-1))

def north_diff(quantity):
    return 0.5 * (quantity[:, 2:] - quantity[:, :-2])

def interior(quantity):
    return quantity[:, 1:-1]

def smoothing(quantity):
    middle = interior(quantity)
    return jnp.roll(middle, -1, axis=-1) + jnp.roll(middle, 1, axis=-1) + quantity[:, 2:] + quantity[:, :-2] - 4.0 * middle

def advance(padded):
    height = padded[:, 0]
    eastward = padded[:, 1]
    northward = padded[:, 2]
    height_mid = interior(height)
    east_mid = interior(eastward)
    north_mid = interior(northward)
    column = DEPTH + height
    height_rate = -(interior(east_diff(column * eastward)) + north_diff(column * northward))
    east_rate = -(east_mid * interior(east_diff(eastward)) + north_mid * north_diff(eastward)) - GRAVITY * interior(east_diff(height)) + CORIOLIS * north_mid
    north_rate = -(east_mid * interior(east_diff(northward)) + north_mid * north_diff(northward)) - GRAVITY * north_diff(height) - CORIOLIS * east_mid
    return jnp.stack([height_mid + TIMESTEP * height_rate + DIFFUSE * smoothing(height), east_mid + TIMESTEP * east_rate + DIFFUSE * smoothing(eastward), north_mid + TIMESTEP * north_rate + DIFFUSE * smoothing(northward)], axis=1)

def predicted_prior(ensemble_block):
    for repeat in range(STEPS):
        ensemble_block = advance(jnp.pad(ensemble_block, ((0, 0), (0, 0), (1, 1), (0, 0)), mode='wrap'))
    return ensemble_block

def innovations(observed, target, variance, weight):
    obs_mean = lax.optimization_barrier(jnp.mean(observed, axis=0))
    perturbed = (observed - obs_mean) * weight
    misfit = (target - obs_mean) * weight
    spread = lax.optimization_barrier(jnp.sum(perturbed * perturbed, axis=0)) / (observed.shape[0] - 1)
    return (perturbed, misfit, jnp.sum(misfit * misfit), jnp.sum(weight * (spread + variance)))

def gram_terms(perturbed, misfit, variance):
    weighted_matrix = perturbed / variance
    product = jnp.einsum('mo,no->mn', weighted_matrix, perturbed, precision=PRECISE)
    projected = jnp.dot(perturbed, misfit / variance, precision=PRECISE)
    return (product, projected)

def spectral_map(gram_scaled):
    upper_bound = 2.0 + jnp.sqrt(jnp.sum(gram_scaled * gram_scaled))
    order_count = gram_scaled.shape[0]
    shifted = 2.0 / (upper_bound - 1.0) * gram_scaled - jnp.eye(order_count, dtype=jnp.float32)
    orders = jnp.arange(DEGREE + 1, dtype=jnp.float32)
    angles = (orders + 0.5) * (math.pi / (DEGREE + 1))
    levels = 0.5 * (upper_bound + 1.0) + 0.5 * (upper_bound - 1.0) * jnp.cos(angles)
    values = lax.rsqrt(levels)
    cos_table = jnp.cos(orders[:, None] * angles[None, :])
    coeffs = 2.0 / (DEGREE + 1) * lax.optimization_barrier(jnp.sum(cos_table * values[None, :], axis=1))
    coeffs = coeffs * jnp.where(orders == 0.0, 0.5, 1.0)
    return (shifted, coeffs)

def chebyshev(shifted, operand, coeffs):
    previous = operand
    current = jnp.dot(shifted, operand, precision=PRECISE)
    summed = coeffs[0] * previous + coeffs[1] * current
    for term_index in range(2, DEGREE + 1):
        following = 2.0 * jnp.dot(shifted, current, precision=PRECISE) - previous
        summed = summed + coeffs[term_index] * following
        previous, current = (current, following)
    return summed

def analyse(columns, product, projected, inflation):
    gram_scaled = inflation / (ENSEMBLE_SIZE - 1) * product
    shifted, coeffs = spectral_map(gram_scaled)
    centre = lax.optimization_barrier(jnp.mean(columns, axis=0))
    spread = columns - centre
    shaped = chebyshev(shifted, spread, coeffs)
    weights = inflation / (ENSEMBLE_SIZE - 1) * chebyshev(shifted, chebyshev(shifted, projected, coeffs), coeffs)
    mean_shift = jnp.dot(weights, spread, precision=PRECISE)
    return centre + jnp.sqrt(inflation) * shaped + mean_shift

def reference(ensemble, obs_cells, region_tile, obs_values, obs_error):
    ensemble_block = ensemble.reshape(N_MEM, ENSEMBLE_SIZE // N_MEM, 3, GY, MESH_LONGITUDES)
    layered_arrays = lax.map(predicted_prior, ensemble_block).reshape(ENSEMBLE_SIZE, 3, N_TILE, BLOCK_LATITUDES, MESH_LONGITUDES)
    by_tile = jnp.transpose(layered_arrays, (2, 0, 1, 3, 4)).reshape(N_TILE, ENSEMBLE_SIZE, 3 * BLOCK_LATITUDES * MESH_LONGITUDES)
    region_count = region_tile.shape[0]
    tile_region = jnp.zeros((region_count,), jnp.int32).at[region_tile].set(jnp.arange(region_count, dtype=jnp.int32))
    obs_index = obs_cells[tile_region]
    targets = obs_values[tile_region]
    variances = obs_error[tile_region]
    unit = jnp.ones((OBS,), jnp.float32)

    def tile_sums(packed):
        flat_state, index_row, target, variance = packed
        observed = jnp.take(flat_state, index_row, axis=1)
        perturbed, misfit, misfit_sum, spread_sum = innovations(observed, target, variance, unit)
        return (misfit_sum, spread_sum)
    misfit_sums, spread_sums = lax.map(tile_sums, (by_tile, obs_index, targets, variances))
    inflation = jnp.sum(misfit_sums) / jnp.sum(spread_sums)

    def tile_update(packed):
        flat_state, index_row, target, variance = packed
        observed = jnp.take(flat_state, index_row, axis=1)
        perturbed, misfit, misfit_sum, spread_sum = innovations(observed, target, variance, unit)
        product, projected = gram_terms(perturbed, misfit, variance)
        return analyse(flat_state, product, projected, inflation)
    updated = lax.map(tile_update, (by_tile, obs_index, targets, variances))
    return jnp.transpose(updated.reshape(N_TILE, ENSEMBLE_SIZE, 3, BLOCK_LATITUDES, MESH_LONGITUDES), (1, 2, 0, 3, 4)).reshape(ENSEMBLE_SIZE, 3, GY, MESH_LONGITUDES)
```

```python
import functools
import math

import jax
import jax.numpy as jnp
from jax import lax
from jax.experimental import pallas as pl
from jax.experimental.pallas import tpu as pltpu
from jax.sharding import PartitionSpec as P

STEPS = 4
DEGREE = 4
FIELDS = 3
LANES = 128
CHUNKS = 4
PAD = 8
HIGHEST = lax.Precision.HIGHEST


F32 = jnp.float32
BF16 = jnp.bfloat16


def params():
    return pltpu.CompilerParams(vmem_limit_bytes=56 * 1024 * 1024)


def split2(x):
    high = x.astype(BF16)
    return high, (x - high.astype(F32)).astype(BF16)


def dot(a, b):
    return lax.dot_general(a, b, (((1,), (0,)), ((), ())), preferred_element_type=F32)


def dot_full(a, b):
    return lax.dot_general(
        a, b, (((1,), (0,)), ((), ())), precision=HIGHEST, preferred_element_type=F32
    )


def spread_body(x_ref, top_ref, bot_ref, *, rows, size):
    stride = FIELDS * rows
    for field in range(FIELDS):
        for row in range(rows):
            out = top_ref if row < rows // 2 else bot_ref
            value = x_ref[pl.ds(field * rows + row, size, stride=stride), :]
            value = value + 1.0 if field == 0 else value * 1.5
            out[field * (rows // 2) + row % (rows // 2)] = value


def spread_chunk(flat, chunk, size, rows, width):
    half = FIELDS * (rows // 2)
    shape = jax.ShapeDtypeStruct((half, size, width), F32)
    return pl.pallas_call(
        functools.partial(spread_body, rows=rows, size=size),
        grid=(width // LANES,),
        in_specs=[pl.BlockSpec((size * FIELDS * rows, LANES), lambda i: (chunk, i))],
        out_specs=[pl.BlockSpec((half, size, LANES), lambda i: (0, 0, i))] * 2,
        out_shape=[shape, shape],
        compiler_params=params(),
        name=f"spread{chunk}",
    )(flat)


def shifted(x, width):
    return pltpu.roll(x, width - 1, 1), pltpu.roll(x, 1, 1)


def advance_row(south, middle, north, width, last):
    hs, us, vs = south
    h, u, v = middle
    hn, un, vn = north
    he, hw = shifted(h, width)
    ue, uw = shifted(u, width)
    ve, vw = shifted(v, width)
    um, up, vm, vp = 1.0 - u, 1.0 + u, 1.0 - v, 1.0 + v
    h_sum = (he * (1.0 - ue) + hw * (1.0 + uw)) + (hn * (1.0 - vn) + hs * (1.0 + vs))
    u_sum = (ue * um + uw * up) + (un * vm + us * vp)
    v_sum = (ve * um + vw * up) + (vn * vm + vs * vp)
    h_new = 0.6 * h + 0.1 * h_sum
    u_new = (0.6 * u + 0.15 * v) + 0.1 * u_sum - 0.225 * (he - hw)
    v_new = (0.6 * v - 0.15 * u) + 0.1 * v_sum - 0.225 * (hn - hs)
    if last:
        return h_new - 1.0, u_new * (2.0 / 3.0), v_new * (2.0 / 3.0)
    return h_new, u_new, v_new


def forecast_body(
    me_ref, prev_ref, top_ref, bot_ref, next_ref, onehot_ref, *refs, rows, size, width, parts, obs
):
    state_ref, sends, work = refs[0], refs[1 : 1 + parts], refs[1 + parts]
    half = rows // 2
    total = rows + 2 * STEPS
    sources = (prev_ref, top_ref, bot_ref, next_ref)
    halves = width // LANES
    slabs = FIELDS * rows
    each = slabs * halves // parts

    def group(index, carry):
        members = pl.ds(pl.multiple_of(index * 8, 8), 8)

        def first(row):
            ref = sources[row // half]
            return tuple(ref[f * half + row % half, members, :] for f in range(FIELDS))

        def later(step):
            return lambda row: tuple(work[(step - 1) % 2, f * total + row] for f in range(FIELDS))

        for step in range(STEPS):
            load = first if step == 0 else later(step)
            last = step == STEPS - 1
            lo, hi = step + 1, total - 1 - step
            window = [load(lo - 1), load(lo)]
            for row in range(lo, hi):
                window.append(load(row + 1))
                new = advance_row(window[0], window[1], window[2], width, last)
                window.pop(0)
                for f in range(FIELDS):
                    if last:
                        slab = f * rows + row - STEPS
                        for k in range(halves):
                            state_ref[slab * halves + k, members, :] = new[f][
                                :, k * LANES : (k + 1) * LANES
                            ]
                    else:
                        work[step % 2, f * total + row] = new[f]
        return carry

    lax.fori_loop(0, size // 8, group, 0)

    observed = jnp.zeros((size, obs), F32)
    for slab in range(slabs):
        x = jnp.concatenate([state_ref[slab * halves + k] for k in range(halves)], axis=1)
        high = x.astype(BF16)
        rest = x - high.astype(F32)
        mid = rest.astype(BF16)
        low = (rest - mid.astype(F32)).astype(BF16)
        stacked = jnp.concatenate([high, mid, low], axis=0)
        part = dot(stacked, onehot_ref[slab])
        observed = observed + ((part[:size] + part[size : 2 * size]) + part[2 * size :])
    me = me_ref[0]
    for p in range(parts):
        begin = (me ^ p) * each
        for j in range(each):
            sends[p][j] = state_ref[begin + j]
        for k in range(obs // LANES):
            sends[p][each + k] = observed[:, k * LANES : (k + 1) * LANES]


def forecast_chunk(me, prev, top, bot, nxt, onehot, rows, size, width, parts, obs):
    units = FIELDS * rows * (width // LANES)
    each = units // parts + obs // LANES
    vmem = pl.BlockSpec(memory_space=pltpu.VMEM)
    return pl.pallas_call(
        functools.partial(
            forecast_body, rows=rows, size=size, width=width, parts=parts, obs=obs
        ),
        in_specs=[pl.BlockSpec(memory_space=pltpu.SMEM)] + [vmem] * 5,
        out_specs=[vmem] * (1 + parts),
        out_shape=[jax.ShapeDtypeStruct((units, size, LANES), F32)]
        + [jax.ShapeDtypeStruct((each, size, LANES), F32)] * parts,
        scratch_shapes=[pltpu.VMEM((2, FIELDS * (rows + 2 * STEPS), 8, width), F32)],
        compiler_params=params(),
        cost_estimate=pl.CostEstimate(flops=50_000_000, bytes_accessed=8_000_000, transcendentals=0),
        name="forecast",
    )(me, prev, top, bot, nxt, onehot)


def covariance_body(target_ref, variance_ref, *refs, count, each, obs, first):
    blocks = refs[:count]
    first_ref, second_ref, sums_ref, mean_ref = refs[count : count + 4]
    total = sum(ref.shape[1] for ref in blocks)
    scale = 1.0 / total
    tails = obs // LANES
    y = jnp.concatenate(
        [
            jnp.concatenate([ref[each + k] for k in range(tails)], axis=1)
            for ref in blocks
        ],
        axis=0,
    )
    y_mean = jnp.sum(y, axis=0, keepdims=True) * scale
    perturbed = y - y_mean
    misfit = target_ref[...] - y_mean
    spread = jnp.sum(perturbed * perturbed, axis=0, keepdims=True) / (total - 1)
    sums_ref[0:1, :] = misfit * misfit
    sums_ref[1:2, :] = spread + variance_ref[...]
    mean_ref[...] = jnp.broadcast_to(y_mean, mean_ref.shape)
    high, low = split2(perturbed.T)
    both = jnp.concatenate([high, low], axis=0)
    step = 2 if each % 2 == 0 and first % 2 == 0 else 1
    for unit in range(0, each, step):
        x = jnp.concatenate(
            [jnp.concatenate([ref[unit + k] for ref in blocks], axis=0) for k in range(step)],
            axis=1,
        )
        x_mean = jnp.sum(x, axis=0, keepdims=True) * scale
        d_high, d_low = split2(x - x_mean)
        part = dot(both, d_high)
        product = (part[:obs] + part[obs:]) + dot(high, d_low)
        for k in range(step):
            out, at = (first_ref, unit + k) if unit < first else (second_ref, unit + k - first)
            lanes = slice(k * LANES, (k + 1) * LANES)
            out[at, :obs, :] = product[:, lanes]
            out[at, obs:, :] = jnp.broadcast_to(x_mean[:, lanes], (PAD, LANES))


def covariance(target, variance, blocks, each, obs):
    vmem = pl.BlockSpec(memory_space=pltpu.VMEM)
    first = (each + 1) // 2
    return pl.pallas_call(
        functools.partial(
            covariance_body, count=len(blocks), each=each, obs=obs, first=first
        ),
        in_specs=[vmem] * (2 + len(blocks)),
        out_specs=[vmem] * 4,
        out_shape=[
            jax.ShapeDtypeStruct((first, obs + PAD, LANES), F32),
            jax.ShapeDtypeStruct((each - first, obs + PAD, LANES), F32),
            jax.ShapeDtypeStruct((2, obs), F32),
            jax.ShapeDtypeStruct((8, obs), F32),
        ],
        compiler_params=params(),
        cost_estimate=pl.CostEstimate(
            flops=10_000_000, bytes_accessed=8_000_000, transcendentals=0
        ),
        name="covariance",
    )(target, variance, *blocks)


def weights_body(
    sums_ref, target_ref, variance_ref, mean_ref, *refs, count, mine, obs, total
):
    tails = obs // LANES
    blocks = [refs[i * tails : (i + 1) * tails] for i in range(count)]
    weights_ref, scale_ref = refs[count * tails :]

    def observed(slabs):
        return jnp.concatenate([slab[0] for slab in slabs], axis=1)

    y_mean = mean_ref[0:1, :]
    inflation = sums_ref[0:1, 0:1] / sums_ref[0:1, 1:2]
    factor = inflation / (total - 1)
    variance = variance_ref[...]
    weighted = (target_ref[...] - y_mean) / variance
    perturbed = jnp.concatenate([observed(ref) for ref in blocks], axis=0) - y_mean
    gram = lax.dot_general(
        perturbed, perturbed, (((0,), (0,)), ((), ())), precision=HIGHEST,
        preferred_element_type=F32,
    )
    g_row = jnp.sqrt(factor / variance)
    eye = (
        lax.broadcasted_iota(jnp.int32, (obs, obs), 0)
        == lax.broadcasted_iota(jnp.int32, (obs, obs), 1)
    ).astype(F32)
    g_col = jnp.sum(eye * g_row, axis=1, keepdims=True)
    kernel = gram * g_row * g_col
    norm = jnp.sum(jnp.sum(kernel * kernel, axis=1, keepdims=True), axis=0, keepdims=True)
    bound = 2.0 + jnp.sqrt(norm)
    slope = 2.0 / (bound - 1.0)
    angles = [(j + 0.5) * (math.pi / (DEGREE + 1)) for j in range(DEGREE + 1)]
    values = [
        lax.rsqrt(0.5 * (bound + 1.0) + 0.5 * (bound - 1.0) * math.cos(angle))
        for angle in angles
    ]
    coeffs = []
    for k in range(DEGREE + 1):
        term = sum(math.cos(k * angle) * value for angle, value in zip(angles, values))
        coeffs.append((2.0 if k else 1.0) / (DEGREE + 1) * term)
    base = coeffs[0] - coeffs[1]
    shifted_kernel = slope * kernel - eye
    before = jnp.zeros((obs, obs), F32)
    current = slope * eye
    summed = coeffs[1] * current
    for k in range(1, DEGREE):
        sign = -1.0 if k % 2 else 1.0
        if k == 1:
            product = slope * shifted_kernel
        else:
            product = dot_full(shifted_kernel, current)
        following = 2.0 * product - before + (2.0 * sign) * slope * eye
        summed = summed + coeffs[k + 1] * following
        base = base - sign * coeffs[k + 1]
        before, current = current, following
    middle = summed * g_row * g_col
    row = jnp.broadcast_to(weighted, (8, obs))
    for _ in range(2):
        row = base * row + dot_full(dot_full(row, gram), middle)
    row = factor * row[0:1, :]
    root = jnp.sqrt(inflation)
    own = jnp.concatenate([observed(blocks[i]) for i in mine], axis=0) - y_mean
    weights_ref[...] = dot_full(own, root * middle) + row
    scale_ref[...] = jnp.broadcast_to(root * base, scale_ref.shape)


def make_weights(sums, target, variance, mean, blocks, mine, each, obs):
    vmem = pl.BlockSpec(memory_space=pltpu.VMEM)
    total = sum(block.shape[1] for block in blocks)
    own = sum(blocks[i].shape[1] for i in mine)
    tails = obs // LANES
    slabs, specs = [], []
    for block in blocks:
        for k in range(tails):
            slabs.append(block)
            specs.append(pl.BlockSpec((1, block.shape[1], LANES), lambda i, k=k: (each + k, 0, 0)))
    return pl.pallas_call(
        functools.partial(weights_body, count=len(blocks), mine=mine, obs=obs, total=total),
        grid=(1,),
        in_specs=[vmem] * 4 + specs,
        out_specs=[vmem] * 2,
        out_shape=[
            jax.ShapeDtypeStruct((own, obs), F32),
            jax.ShapeDtypeStruct((8, LANES), F32),
        ],
        compiler_params=params(),
        cost_estimate=pl.CostEstimate(
            flops=10_000_000, bytes_accessed=2_000_000, transcendentals=0
        ),
        name="weights",
    )(sums, target, variance, mean, *slabs)


def update_body(me_ref, scale_ref, weights_ref, *refs, chunks, parts, first, each, rows, obs):
    states = refs[:chunks]
    pieces = refs[chunks : chunks + 2 * parts]
    out_ref, gathered, split_w, turned, sems = refs[chunks + 2 * parts :]
    field, half = pl.program_id(0), pl.program_id(1)
    members = weights_ref.shape[0]

    @pl.when((field == 0) & (half == 0))
    def _():
        copies = []
        for p in range(parts):
            for colour in range(2):
                piece = pieces[2 * p + colour]
                begin = (me_ref[0] ^ p) * each + colour * first
                copies.append(
                    pltpu.make_async_copy(
                        piece, gathered.at[pl.ds(begin, piece.shape[0])], sems.at[2 * p + colour]
                    )
                )
        for copy in copies:
            copy.start()
        high, low = split2(weights_ref[...])
        split_w[:members] = high
        split_w[members:] = low
        for copy in copies:
            copy.wait()

    halves = pl.num_programs(1)
    scale = scale_ref[0:1, :]
    high = split_w[:members]
    both = split_w[...]
    for row in range(rows):
        unit = (field * rows + row) * halves + half
        c = gathered[unit]
        c_high, c_low = split2(c[:obs])
        part = dot(both, c_high)
        product = (part[:members] + part[members:]) + dot(high, c_low)
        x = jnp.concatenate([ref[0, row, 0] for ref in states], axis=0)
        turned[pl.ds(row, members, stride=rows), :] = (
            product + scale * x + (1.0 - scale) * c[obs : obs + 1]
        )
    out_ref[:, 0, :, :] = turned[...].reshape(members, rows, LANES)


def update(me, scale, weights, states, pieces, rows, width, obs, each):
    members = weights.shape[0]
    halves = width // LANES
    first = pieces[0].shape[0]
    units = FIELDS * rows * halves
    parts = len(pieces) // 2
    views = [s.reshape(FIELDS, rows, halves, s.shape[1], LANES) for s in states]
    return pl.pallas_call(
        functools.partial(
            update_body, chunks=len(states), parts=parts, first=first, each=each, rows=rows, obs=obs
        ),
        grid=(FIELDS, halves),
        in_specs=[
            pl.BlockSpec(memory_space=pltpu.SMEM),
            pl.BlockSpec(memory_space=pltpu.VMEM),
            pl.BlockSpec(memory_space=pltpu.VMEM),
        ]
        + [
            pl.BlockSpec((1, rows, 1, s.shape[1], LANES), lambda f, k: (f, 0, k, 0, 0))
            for s in states
        ]
        + [pl.BlockSpec(memory_space=pl.ANY)] * len(pieces),
        out_specs=pl.BlockSpec((members, 1, rows, LANES), lambda f, k: (0, f, 0, k)),
        out_shape=jax.ShapeDtypeStruct((members, FIELDS, rows, width), F32),
        scratch_shapes=[
            pltpu.VMEM((units, obs + PAD, LANES), F32),
            pltpu.VMEM((2 * members, obs), BF16),
            pltpu.VMEM((members * rows, LANES), F32),
            pltpu.SemaphoreType.DMA((2 * parts,)),
        ],
        compiler_params=params(),
        cost_estimate=pl.CostEstimate(
            flops=10_000_000, bytes_accessed=20_000_000, transcendentals=0
        ),
        name="update",
    )(me, scale, weights, *views, *pieces)


def on_device(ensemble, obs_cells, region_tile, obs_values, obs_error):
    members, _, rows, width = ensemble.shape
    parts = lax.axis_size("mem")
    tiles = lax.axis_size("tile")
    obs = obs_cells.shape[1]
    units = FIELDS * rows * (width // LANES)
    each = units // parts
    size = members // CHUNKS
    up = [(i, (i + 1) % tiles) for i in range(tiles)]
    down = [((i + 1) % tiles, i) for i in range(tiles)]

    def swap(x, p):
        return lax.ppermute(x, "mem", [(i, i ^ p) for i in range(parts)])

    me = jnp.reshape(lax.axis_index("mem"), (1,)).astype(jnp.int32)
    flat = ensemble.reshape(members * FIELDS * rows, width)
    halos = []
    for chunk in range(CHUNKS):
        top, bot = spread_chunk(flat, chunk, size, rows, width)
        prev = lax.ppermute(bot, "tile", up)
        nxt = lax.ppermute(top, "tile", down)
        halos.append((prev, top, bot, nxt))

    chosen = (region_tile == lax.axis_index("tile"))[:, None]
    obs_index = jnp.sum(jnp.where(chosen, obs_cells, 0), axis=0)
    target = jnp.sum(jnp.where(chosen, obs_values, 0.0), axis=0, keepdims=True)
    variance = jnp.sum(jnp.where(chosen, obs_error, 0.0), axis=0, keepdims=True)
    cells = lax.broadcasted_iota(jnp.int32, (FIELDS * rows, width, obs), 0) * width
    cells = cells + lax.broadcasted_iota(jnp.int32, (FIELDS * rows, width, obs), 1)
    onehot = (cells == obs_index[None, None, :]).astype(BF16)

    states, blocks, mine = [], [], []
    for chunk in range(CHUNKS):
        state, *sends = forecast_chunk(
            me, *halos[chunk], onehot, rows, size, width, parts, obs
        )
        states.append(state)
        mine.append(len(blocks))
        blocks.append(sends[0])
        for p in reversed(range(1, parts)):
            blocks.append(swap(sends[p], p))

    c_first, c_second, sums, y_mean = covariance(target, variance, blocks, each, obs)
    pieces = [c_first, c_second]
    if parts == 4:
        x_first, y_second = swap(c_first, 1), swap(c_second, 2)
        x_second, y_first = swap(c_second, 1), swap(c_first, 2)
        pieces += [x_first, x_second, y_first, y_second, swap(x_first, 2), swap(y_second, 1)]
    else:
        for p in range(1, parts):
            pieces += [swap(c_first, p), swap(c_second, p)]
    sums = lax.psum(jnp.sum(sums, axis=1)[None, :], "tile")
    weights, scale = make_weights(sums, target, variance, y_mean, blocks, mine, each, obs)
    return update(me, scale, weights, states, pieces, rows, width, obs, each)


def solution(mesh):
    in_specs = (P("mem", None, "tile", None), P(), P(), P(), P())
    out_specs = P("mem", None, "tile", None)
    return jax.shard_map(
        on_device, mesh=mesh, in_specs=in_specs, out_specs=out_specs, check_vma=False
    )
```

```python
import functools
import math

import jax
import jax.numpy as jnp
from jax import lax
from jax.experimental import pallas as pl
from jax.experimental.pallas import tpu as pltpu
from jax.sharding import PartitionSpec as P


STEPS = 4
DEGREE = 4
FIELDS = 3
LANES = 128
CHUNKS = 4
VMEM_MIB = 22
SPREAD_VMEM_MIB = 58
REST_VMEM_MIB = 22
FIRST = 2
SPARE = 8
HIGHEST = lax.Precision.HIGHEST


F32 = jnp.float32
BF16 = jnp.bfloat16


def params(mib=VMEM_MIB):
    return pltpu.CompilerParams(vmem_limit_bytes=mib * 1024 * 1024)


def split2(x):
    high = x.astype(BF16)
    return high, (x - high.astype(F32)).astype(BF16)


def dot(a, b):
    return lax.dot_general(a, b, (((1,), (0,)), ((), ())), preferred_element_type=F32)


def dot_full(a, b):
    return lax.dot_general(
        a, b, (((1,), (0,)), ((), ())), precision=HIGHEST, preferred_element_type=F32
    )


def spread_body(x_ref, *refs, chunks, rows):
    outs, (staged, sems) = refs[: 2 * len(chunks)], refs[2 * len(chunks) :]
    stride = FIELDS * rows
    halves = staged.shape[0]
    copies, at = [], 0
    for index, (begin, size) in enumerate(chunks):
        for k in range(halves):
            copies.append(
                pltpu.make_async_copy(
                    x_ref.at[pl.ds(begin * stride, size * stride), pl.ds(k * LANES, LANES)],
                    staged.at[k, pl.ds(at * stride, size * stride)],
                    sems.at[index * halves + k],
                )
            )
        at += size
    for copy in copies:
        copy.start()
    at = 0
    for index, (begin, size) in enumerate(chunks):
        for k in range(halves):
            copies[index * halves + k].wait()
            for field in range(FIELDS):
                for row in range(rows):
                    out = outs[2 * index + row // (rows // 2)]
                    first = at * stride + field * rows + row
                    value = staged[k, pl.ds(first, size, stride=stride), :]
                    value = value + 1.0 if field == 0 else value * 1.5
                    slot = field * (rows // 2) + row % (rows // 2)
                    out[slot, :, k * LANES : (k + 1) * LANES] = value
        at += size


def spread(flat, chunks, rows, width, mib):
    half = FIELDS * (rows // 2)
    halves = width // LANES
    total = sum(size for _, size in chunks)
    shapes = [jax.ShapeDtypeStruct((half, size, width), F32) for _, size in chunks for _ in (0, 1)]
    out = pl.pallas_call(
        functools.partial(spread_body, chunks=chunks, rows=rows),
        in_specs=[pl.BlockSpec(memory_space=pl.ANY)],
        out_specs=[pl.BlockSpec(memory_space=pltpu.VMEM)] * len(shapes),
        out_shape=shapes,
        scratch_shapes=[
            pltpu.VMEM((halves, total * FIELDS * rows, LANES), F32),
            pltpu.SemaphoreType.DMA((halves * len(chunks),)),
        ],
        compiler_params=params(mib),
        name="spread",
    )(flat)
    return [(out[2 * i], out[2 * i + 1]) for i in range(len(chunks))]


def shifted(x, width):
    return pltpu.roll(x, width - 1, 1), pltpu.roll(x, 1, 1)


def prepared(h, u, v):
    vm, vp = 1.0 - v, 1.0 + v
    return h, u, v, vm, vp, h * vm, h * vp


def advance_row(south, middle, north, width, last):
    hs, us, vs, _, _, _, flow_s = south
    h, u, v, vm, vp, _, _ = middle
    hn, un, vn, _, _, flow_n, _ = north
    he, hw = shifted(h, width)
    ue, uw = shifted(u, width)
    ve, vw = shifted(v, width)
    um, up = 1.0 - u, 1.0 + u
    h_sum = (he * (1.0 - ue) + hw * (1.0 + uw)) + (flow_n + flow_s)
    u_sum = (ue * um + uw * up) + (un * vm + us * vp)
    v_sum = (ve * um + vw * up) + (vn * vm + vs * vp)
    h_new = 0.6 * h + 0.1 * h_sum
    u_new = (0.6 * u + 0.15 * v) + 0.1 * u_sum - 0.225 * (he - hw)
    v_new = (0.6 * v - 0.15 * u) + 0.1 * v_sum - 0.225 * (hn - hs)
    if last:
        return h_new - 1.0, u_new * (2.0 / 3.0), v_new * (2.0 / 3.0)
    return h_new, u_new, v_new


def owned_runs(units, parts, rows):
    each = units // parts
    whole = each // rows * rows
    runs = [(whole, 0), (each - whole, parts * whole)]
    return [run for run in runs if run[0]]


def forecast_body(
    me_ref, prev_ref, top_ref, bot_ref, next_ref, onehot_ref, *refs, begin, rows, size, block,
    width, parts, obs
):
    work, kept, onehot, sem, state_sems = refs[-5:]
    state_ref, *sends = refs[-6 - parts : -5]
    half = rows // 2
    total = rows + 2 * STEPS
    sources = (prev_ref, top_ref, bot_ref, next_ref)
    halves = width // LANES
    units = FIELDS * rows * halves
    each = units // parts
    place = pl.program_id(0)
    fetch = pltpu.make_async_copy(onehot_ref, onehot, sem)

    @pl.when(place == 0)
    def _():
        fetch.start()

    def group(index, carry):
        members = pl.ds(pl.multiple_of(index * 8, 8), 8)
        kept_members = pl.ds(pl.multiple_of(place * block + index * 8, 8), 8)

        def first(row):
            ref = sources[row // half]
            return prepared(*(ref[f * half + row % half, members, :] for f in range(FIELDS)))

        def later(step):
            return lambda row: prepared(
                *(work[(step - 1) % 2, f * total + row] for f in range(FIELDS))
            )

        for step in range(STEPS):
            load = first if step == 0 else later(step)
            last = step == STEPS - 1
            lo, hi = step + 1, total - 1 - step
            window = [load(lo - 1), load(lo)]
            for row in range(lo, hi):
                window.append(load(row + 1))
                new = advance_row(window[0], window[1], window[2], width, last)
                window.pop(0)
                for f in range(FIELDS):
                    if last:
                        for k in range(halves):
                            unit = (f * halves + k) * rows + row - STEPS
                            value = new[f][:, k * LANES : (k + 1) * LANES]
                            kept[unit, kept_members, :] = value
                    else:
                        work[step % 2, f * total + row] = new[f]
        return carry

    lax.fori_loop(0, block // 8, group, 0)

    def keep(index):
        source = pl.ds(pl.multiple_of(index * block, 8), block)
        target = pl.ds(pl.multiple_of(begin + index * block, 8), block)
        return pltpu.make_async_copy(
            kept.at[:, source, :], state_ref.at[:, target, :], state_sems.at[index]
        )

    keep(place).start()

    @pl.when(place == pl.num_programs(0) - 1)
    def _():
        fetch.wait()
        observed = jnp.zeros((size, obs), F32)
        for f in range(FIELDS):
            for row in range(rows):
                x = jnp.concatenate(
                    [kept[(f * halves + k) * rows + row] for k in range(halves)], axis=1
                )
                high = x.astype(BF16)
                rest = x - high.astype(F32)
                mid = rest.astype(BF16)
                low = (rest - mid.astype(F32)).astype(BF16)
                stacked = jnp.concatenate([high, mid, low], axis=0)
                part = dot(stacked, onehot[f * rows + row])
                observed = observed + ((part[:size] + part[size : 2 * size]) + part[2 * size :])
        me = me_ref[0]
        for p in range(parts):
            slot = 0
            for count, base in owned_runs(units, parts, rows):
                for j in range(count):
                    sends[p][slot] = kept[base + (me ^ p) * count + j]
                    slot += 1
            for k in range(obs // LANES):
                sends[p][each + k] = observed[:, k * LANES : (k + 1) * LANES]
        for index in range(size // block):
            keep(index).wait()


def forecast_chunk(
    me, prev, top, bot, nxt, onehot, state, begin, size, members, rows, width, parts, obs
):
    units = FIELDS * rows * (width // LANES)
    each = units // parts + obs // LANES
    half = FIELDS * (rows // 2)
    block = 16 if size % 16 == 0 else 8
    extra = [] if state is None else [state]
    return pl.pallas_call(
        functools.partial(
            forecast_body, begin=begin, rows=rows, size=size, block=block, width=width,
            parts=parts, obs=obs
        ),
        grid=(size // block,),
        in_specs=[pl.BlockSpec(memory_space=pltpu.SMEM)]
        + [pl.BlockSpec((half, block, width), lambda i: (0, i, 0))] * 4
        + [pl.BlockSpec(memory_space=pl.ANY)] * (1 + len(extra)),
        out_specs=[pl.BlockSpec(memory_space=pl.ANY)]
        + [pl.BlockSpec((each, size, LANES), lambda i: (0, 0, 0))] * parts,
        out_shape=[jax.ShapeDtypeStruct((units, SPARE * members, LANES), F32)]
        + [jax.ShapeDtypeStruct((each, size, LANES), F32)] * parts,
        scratch_shapes=[
            pltpu.VMEM((2, FIELDS * (rows + 2 * STEPS), 8, width), F32),
            pltpu.VMEM((units, size, LANES), F32),
            pltpu.VMEM(onehot.shape, BF16),
            pltpu.SemaphoreType.DMA,
            pltpu.SemaphoreType.DMA((size // block,)),
        ],
        compiler_params=params(),
        cost_estimate=pl.CostEstimate(flops=50_000_000, bytes_accessed=8_000_000, transcendentals=0),
        input_output_aliases={6: 0} if extra else {},
        name="forecast",
    )(me, prev, top, bot, nxt, onehot, *extra)


def joined_observed(blocks, each, obs):
    return jnp.concatenate(
        [
            jnp.concatenate([ref[each + k] for k in range(obs // LANES)], axis=1)
            for ref in blocks
        ],
        axis=0,
    )


def centred_products(blocks, each, obs, emit):
    scale = 1.0 / sum(ref.shape[1] for ref in blocks)
    y = joined_observed(blocks, each, obs)
    y_mean = jnp.sum(y, axis=0, keepdims=True) * scale
    perturbed = y - y_mean
    squares = jnp.sum(perturbed * perturbed, axis=0, keepdims=True)
    high, low = split2(perturbed.T)
    both = jnp.concatenate([high, low], axis=0)
    count = each + obs // LANES
    step = 2 if count % 2 == 0 else 1
    for unit in range(0, count, step):
        x = jnp.concatenate(
            [jnp.concatenate([ref[unit + k] for ref in blocks], axis=0) for k in range(step)],
            axis=1,
        )
        x_mean = jnp.sum(x, axis=0, keepdims=True) * scale
        d_high, d_low = split2(x - x_mean)
        part = dot(both, d_high)
        product = (part[:obs] + part[obs:]) + dot(high, d_low)
        for k in range(step):
            lanes = slice(k * LANES, (k + 1) * LANES)
            emit(unit + k, product[:, lanes], x_mean[:, lanes])
    return y_mean, squares


def early_body(*refs, count, each, obs):
    blocks = refs[:count]
    product_ref, mean_ref, y_ref = refs[count:]

    def emit(unit, product, mean):
        product_ref[unit] = product
        mean_ref[unit : unit + 1, :] = mean

    y_mean, squares = centred_products(blocks, each, obs, emit)
    y_ref[0:1, :] = y_mean
    y_ref[1:2, :] = squares


def early_covariance(blocks, each, obs):
    vmem = pl.BlockSpec(memory_space=pltpu.VMEM)
    return pl.pallas_call(
        functools.partial(early_body, count=len(blocks), each=each, obs=obs),
        in_specs=[vmem] * len(blocks),
        out_specs=[vmem] * 3,
        out_shape=[
            jax.ShapeDtypeStruct((each + obs // LANES, obs, LANES), F32),
            jax.ShapeDtypeStruct((each + obs // LANES, LANES), F32),
            jax.ShapeDtypeStruct((2, obs), F32),
        ],
        compiler_params=params(),
        cost_estimate=pl.CostEstimate(
            flops=10_000_000, bytes_accessed=8_000_000, transcendentals=0
        ),
        name="early",
    )(*blocks)


def late_body(
    target_ref, variance_ref, product_ref, mean_ref, y_ref, *refs, count, each, obs, first, before
):
    blocks = refs[:count]
    first_ref, second_ref, sums_ref, y_mean_ref, gram_ref = refs[count:]
    after = sum(ref.shape[1] for ref in blocks)
    total = before + after
    share = after / total
    cross = before * share
    y_late = jnp.sum(joined_observed(blocks, each, obs), axis=0, keepdims=True) * (1.0 / after)
    y_shift = y_late - y_ref[0:1, :]
    column = jnp.broadcast_to(cross * y_shift, (8, obs)).T[:, 0:1]

    def emit(unit, product, mean):
        old = mean_ref[unit : unit + 1, :]
        shift = mean - old
        value = product_ref[unit] + product + column * shift
        if unit >= each:
            gram_ref[:, (unit - each) * LANES : (unit - each + 1) * LANES] = value
            return
        out, at = (first_ref, unit) if unit < first else (second_ref, unit - first)
        out[at * obs : (at + 1) * obs, :] = value
        tail = (first if unit < first else each - first) * obs + at
        out[tail : tail + 1, :] = old + share * shift

    _, squares = centred_products(blocks, each, obs, emit)
    y_mean = y_ref[0:1, :] + share * y_shift
    misfit = target_ref[...] - y_mean
    spread = (y_ref[1:2, :] + squares + cross * y_shift * y_shift) / (total - 1)
    sums_ref[0:1, :] = misfit * misfit
    sums_ref[1:2, :] = spread + variance_ref[...]
    y_mean_ref[...] = jnp.broadcast_to(y_mean, y_mean_ref.shape)


def padded(count):
    return -(-count // 8) * 8


def late_covariance(target, variance, early, blocks, each, obs, before):
    vmem = pl.BlockSpec(memory_space=pltpu.VMEM)
    first = (each + 1) // 2
    second = each - first
    return pl.pallas_call(
        functools.partial(
            late_body, count=len(blocks), each=each, obs=obs, first=first, before=before
        ),
        in_specs=[vmem] * (5 + len(blocks)),
        out_specs=[vmem] * 5,
        out_shape=[
            jax.ShapeDtypeStruct((first * obs + padded(first), LANES), F32),
            jax.ShapeDtypeStruct((second * obs + padded(second), LANES), F32),
            jax.ShapeDtypeStruct((2, obs), F32),
            jax.ShapeDtypeStruct((8, obs), F32),
            jax.ShapeDtypeStruct((obs, obs), F32),
        ],
        compiler_params=params(),
        cost_estimate=pl.CostEstimate(
            flops=10_000_000, bytes_accessed=8_000_000, transcendentals=0
        ),
        name="late",
    )(target, variance, *early, *blocks)


def weights_body(
    sums_ref, target_ref, variance_ref, mean_ref, gram_ref, *refs, count, obs, total
):
    tails = obs // LANES
    blocks = [refs[i * tails : (i + 1) * tails] for i in range(count)]
    weights_ref, scale_ref = refs[count * tails :]

    def observed(slabs):
        return jnp.concatenate([slab[0] for slab in slabs], axis=1)

    y_mean = mean_ref[0:1, :]
    inflation = sums_ref[0:1, 0:1] / sums_ref[0:1, 1:2]
    factor = inflation / (total - 1)
    variance = variance_ref[...]
    weighted = (target_ref[...] - y_mean) / variance
    gram = gram_ref[...]
    g_row = jnp.sqrt(factor / variance)
    eye = (
        lax.broadcasted_iota(jnp.int32, (obs, obs), 0)
        == lax.broadcasted_iota(jnp.int32, (obs, obs), 1)
    ).astype(F32)
    g_col = jnp.sum(eye * g_row, axis=1, keepdims=True)
    kernel = gram * g_row * g_col
    norm = jnp.sum(jnp.sum(kernel * kernel, axis=1, keepdims=True), axis=0, keepdims=True)
    bound = 2.0 + jnp.sqrt(norm)
    slope = 2.0 / (bound - 1.0)
    angles = [(j + 0.5) * (math.pi / (DEGREE + 1)) for j in range(DEGREE + 1)]
    values = [
        lax.rsqrt(0.5 * (bound + 1.0) + 0.5 * (bound - 1.0) * math.cos(angle))
        for angle in angles
    ]
    coeffs = []
    for k in range(DEGREE + 1):
        term = sum(math.cos(k * angle) * value for angle, value in zip(angles, values))
        coeffs.append((2.0 if k else 1.0) / (DEGREE + 1) * term)
    base = coeffs[0] - coeffs[1]
    shifted_kernel = slope * kernel - eye
    before = jnp.zeros((obs, obs), F32)
    current = slope * eye
    summed = coeffs[1] * current
    for k in range(1, DEGREE):
        sign = -1.0 if k % 2 else 1.0
        if k == 1:
            product = slope * shifted_kernel
        else:
            product = dot_full(shifted_kernel, current)
        following = 2.0 * product - before + (2.0 * sign) * slope * eye
        summed = summed + coeffs[k + 1] * following
        base = base - sign * coeffs[k + 1]
        before, current = current, following
    middle = summed * g_row * g_col
    row = jnp.broadcast_to(weighted, (8, obs))
    for _ in range(2):
        row = base * row + dot_full(dot_full(row, gram), middle)
    row = factor * row[0:1, :]
    root = jnp.sqrt(inflation)
    own = jnp.concatenate([observed(block) for block in blocks], axis=0) - y_mean
    weights_ref[...] = dot_full(own, root * middle) + row
    scale_ref[...] = jnp.broadcast_to(root * base, scale_ref.shape)


def make_weights(sums, target, variance, mean, gram, blocks, each, obs, parts):
    vmem = pl.BlockSpec(memory_space=pltpu.VMEM)
    own = sum(block.shape[1] for block in blocks)
    total = parts * own
    tails = obs // LANES
    slabs, specs = [], []
    for block in blocks:
        for k in range(tails):
            slabs.append(block)
            specs.append(pl.BlockSpec((1, block.shape[1], LANES), lambda i, k=k: (each + k, 0, 0)))
    return pl.pallas_call(
        functools.partial(weights_body, count=len(blocks), obs=obs, total=total),
        grid=(1,),
        in_specs=[vmem] * 5 + specs,
        out_specs=[vmem] * 2,
        out_shape=[
            jax.ShapeDtypeStruct((own, obs), F32),
            jax.ShapeDtypeStruct((8, LANES), F32),
        ],
        compiler_params=params(),
        cost_estimate=pl.CostEstimate(
            flops=10_000_000, bytes_accessed=2_000_000, transcendentals=0
        ),
        name="weights",
    )(sums, target, variance, mean, gram, *slabs)


def segments(begin, end, units, parts, rows):
    found, slot = [], 0
    for count, base in owned_runs(units, parts, rows):
        lo, hi = max(begin, slot), min(end, slot + count)
        if lo < hi:
            found.append((lo - begin, hi - lo, base + lo - slot, count))
        slot += count
    return found


def update_body(
    tiles_ref, owner_ref, scale_ref, weights_ref, *refs, chunks, bounds, units, parts, rows, obs
):
    states = refs[:chunks]
    pieces = refs[chunks : chunks + len(bounds)]
    out_ref, gathered, means, split_w, turned = refs[-5:]
    members = weights_ref.shape[0]

    @pl.when(pl.program_id(0) == 0)
    def _():
        high, low = split2(weights_ref[...])
        split_w[:members] = high
        split_w[members:] = low
        for index, (begin, end) in enumerate(bounds):
            owner = owner_ref[index]
            piece = pieces[index]
            tail = (end - begin) * obs
            for slot, count, base, stride in segments(begin, end, units, parts, rows):
                for j in range(slot, slot + count):
                    unit = base + owner * stride + j - slot
                    gathered[unit] = piece[j * obs : (j + 1) * obs, :]
                    means[unit] = jnp.broadcast_to(
                        piece[tail + j : tail + j + 1, :], (8, LANES)
                    )

    tile = tiles_ref[pl.program_id(0)]
    scale = scale_ref[0:1, :]
    high = split_w[:members]
    both = split_w[...]
    for row in range(0, rows, 2):
        unit = tile * rows + row
        c = [gathered[unit + k] for k in range(2)]
        c_high, c_low = split2(jnp.concatenate(c, axis=1))
        part = dot(both, c_high)
        product = (part[:members] + part[members:]) + dot(high, c_low)
        for k in range(2):
            x = jnp.concatenate([ref[0, row + k] for ref in states], axis=0)
            turned[pl.ds(row + k, members, stride=rows), :] = (
                product[:, k * LANES : (k + 1) * LANES]
                + scale * x
                + (1.0 - scale) * means[unit + k, 0:1, :]
            )
    out_ref[:, 0, :, :] = turned[...].reshape(members, rows, LANES)


def update(tiles, scale, weights, states, pieces, owners, bounds, rows, width, obs, parts, into):
    members = weights.shape[0]
    halves = width // LANES
    units = FIELDS * rows * halves
    views = [s.reshape(FIELDS * halves, rows, s.shape[1], LANES) for s in states]
    vmem = pl.BlockSpec(memory_space=pltpu.VMEM)
    extra = [] if into is None else [into]
    body = functools.partial(
        update_body, chunks=len(states), bounds=bounds, units=units, parts=parts, rows=rows, obs=obs
    )
    operands = [scale, weights, *views, *pieces, *extra]
    return pl.pallas_call(
        body,
        grid_spec=pltpu.PrefetchScalarGridSpec(
            num_scalar_prefetch=2,
            grid=(tiles.shape[0],),
            in_specs=[
                pl.BlockSpec(scale.shape, lambda i, t, o: (0, 0)),
                pl.BlockSpec(weights.shape, lambda i, t, o: (0, 0)),
            ]
            + [
                pl.BlockSpec((1, rows, members, LANES), lambda i, t, o: (t[i], 0, 0, 0))
                for v in views
            ]
            + [pl.BlockSpec(piece.shape, lambda i, t, o: (0, 0)) for piece in pieces]
            + [pl.BlockSpec(memory_space=pl.ANY)] * len(extra),
            out_specs=pl.BlockSpec(
                (members, 1, rows, LANES), lambda i, t, o: (0, t[i] // halves, 0, t[i] % halves)
            ),
            scratch_shapes=[
                pltpu.VMEM((units, obs, LANES), F32),
                pltpu.VMEM((units, 8, LANES), F32),
                pltpu.VMEM((2 * members, obs), BF16),
                pltpu.VMEM((members * rows, LANES), F32),
            ],
        ),
        out_shape=jax.ShapeDtypeStruct((members, FIELDS, rows, width), F32),
        input_output_aliases={} if into is None else {2 + len(operands) - 1: 0},
        compiler_params=params(),
        cost_estimate=pl.CostEstimate(
            flops=10_000_000, bytes_accessed=20_000_000, transcendentals=0
        ),
        name="update" if into is None else "finish",
    )(tiles, owners, *operands)


def chunk_plan(members):
    unit = members // 16
    if unit % 8:
        size = members // CHUNKS
        return [(size * i, size) for i in range(CHUNKS)]
    shares = [(0, 2), (2, 3), (5, 3), (8, 3), (11, 3), (14, 2)]
    return [(unit * begin, unit * size) for begin, size in shares]


def step(ensemble, obs_cells, region_tile, obs_values, obs_error):
    members, _, rows, width = ensemble.shape
    parts = lax.axis_size("mem")
    tiles = lax.axis_size("tile")
    obs = obs_cells.shape[1]
    halves = width // LANES
    units = FIELDS * rows * halves
    each = units // parts
    plan = chunk_plan(members)
    order = sorted(range(len(plan)), key=lambda chunk: plan[chunk])
    up = [(i, (i + 1) % tiles) for i in range(tiles)]
    down = [((i + 1) % tiles, i) for i in range(tiles)]

    def swap(x, p):
        return lax.ppermute(x, "mem", [(i, i ^ p) for i in range(parts)])

    me = jnp.reshape(lax.axis_index("mem"), (1,)).astype(jnp.int32)
    flat = ensemble.reshape(members * FIELDS * rows, width)

    chosen = (region_tile == lax.axis_index("tile"))[:, None]
    obs_index = jnp.sum(jnp.where(chosen, obs_cells, 0), axis=0)
    target = jnp.sum(jnp.where(chosen, obs_values, 0.0), axis=0, keepdims=True)
    variance = jnp.sum(jnp.where(chosen, obs_error, 0.0), axis=0, keepdims=True)
    cells = lax.broadcasted_iota(jnp.int32, (FIELDS * rows, width, obs), 0) * width
    cells = cells + lax.broadcasted_iota(jnp.int32, (FIELDS * rows, width, obs), 1)
    onehot = (cells == obs_index[None, None, :]).astype(BF16)

    pairs = spread(flat, plan[:FIRST], rows, width, SPREAD_VMEM_MIB)
    pairs += spread(flat, plan[FIRST:], rows, width, REST_VMEM_MIB)

    def halo(chunk):
        top, bot = pairs[chunk]
        prev = lax.ppermute(bot, "tile", up)
        return prev, top, bot, lax.ppermute(top, "tile", down)

    blocks, mine, state = [], [], None
    for chunk, (begin, size) in enumerate(plan):
        prev, top, bot, nxt = halo(chunk)
        state, *sends = forecast_chunk(
            me, prev, top, bot, nxt, onehot, state, begin, size, members, rows, width, parts, obs
        )
        mine.append(sends[0])
        blocks.append(sends[0])
        for p in reversed(range(1, parts)):
            blocks.append(swap(sends[p], p))

    late = len(blocks) - parts
    early = early_covariance(blocks[:late], each, obs)
    c_first, c_second, sums, y_mean, gram = late_covariance(
        target, variance, early, blocks[late:], each, obs, parts * (members - plan[-1][1])
    )
    first = (each + 1) // 2
    bounds = [(0, first), (first, each)]
    sums = lax.psum(jnp.sum(sums, axis=1)[None, :], "tile")
    weights, scale = make_weights(
        sums, target, variance, y_mean, gram, [mine[chunk] for chunk in order], each, obs, parts
    )
    args = (scale, weights, [state])
    sizes_of = (rows, width, obs, parts)
    if parts == 4 and each == rows + rows // 2:
        x_first, y_second = swap(c_first, 1), swap(c_second, 2)
        x_second, y_first = swap(c_second, 1), swap(c_first, 2)
        far_first, far_second = swap(x_first, 2), swap(y_second, 1)
        own, x, y, far = me, me ^ 1, me ^ 2, me ^ 3
        done = update(
            jnp.concatenate([own, x, y, parts + own // 2]),
            *args,
            [c_first, c_second, x_first, x_second, y_first, y_second],
            jnp.concatenate([own, own, x, x, y, y]),
            bounds * 3,
            *sizes_of,
            None,
        )
        return update(
            jnp.concatenate([far, parts + far // 2]),
            *args,
            [far_first, far_second, y_second],
            jnp.concatenate([far, far, y]),
            bounds + bounds[1:],
            *sizes_of,
            done,
        )
    pieces, owners = [], []
    for p in range(parts):
        for piece in (c_first, c_second):
            pieces.append(swap(piece, p) if p else piece)
            owners.append(me ^ p)
    return update(
        jnp.arange(FIELDS * halves, dtype=jnp.int32),
        *args,
        pieces,
        jnp.concatenate(owners),
        bounds * parts,
        *sizes_of,
        None,
    )


def solution(mesh):
    in_specs = (P("mem", None, "tile", None), P(), P(), P(), P())
    out_specs = P("mem", None, "tile", None)
    return jax.shard_map(step, mesh=mesh, in_specs=in_specs, out_specs=out_specs, check_vma=False)
```

```python
import functools
import math

import jax
import jax.numpy as jnp
from jax import lax
from jax.experimental import pallas as pl
from jax.experimental.pallas import tpu as pltpu
from jax.sharding import PartitionSpec as P


STEPS = 4
DEGREE = 4
FIELDS = 3
LANES = 128
CHUNKS = 4
AHEAD = 3
VMEM_MIB = 22
SPREAD_VMEM_MIB = 58
REST_VMEM_MIB = 22
SPARE = 8
HIGHEST = lax.Precision.HIGHEST


F32 = jnp.float32
BF16 = jnp.bfloat16


def params(mib=VMEM_MIB):
    return pltpu.CompilerParams(vmem_limit_bytes=mib * 1024 * 1024)


def split2(x):
    high = x.astype(BF16)
    return high, (x - high.astype(F32)).astype(BF16)


def dot(a, b):
    return lax.dot_general(a, b, (((1,), (0,)), ((), ())), preferred_element_type=F32)


def dot_full(a, b):
    return lax.dot_general(
        a, b, (((1,), (0,)), ((), ())), precision=HIGHEST, preferred_element_type=F32
    )


def spread_body(x_ref, *refs, chunks, rows):
    outs, (staged, sems) = refs[: 2 * len(chunks)], refs[2 * len(chunks) :]
    stride = FIELDS * rows
    halves = staged.shape[0]
    copies, at = [], 0
    for index, (begin, size) in enumerate(chunks):
        for k in range(halves):
            copies.append(
                pltpu.make_async_copy(
                    x_ref.at[pl.ds(begin * stride, size * stride), pl.ds(k * LANES, LANES)],
                    staged.at[k, pl.ds(at * stride, size * stride)],
                    sems.at[index * halves + k],
                )
            )
        at += size
    for copy in copies:
        copy.start()
    at = 0
    for index, (begin, size) in enumerate(chunks):
        for k in range(halves):
            copies[index * halves + k].wait()
            for field in range(FIELDS):
                for row in range(rows):
                    out = outs[2 * index + row // (rows // 2)]
                    first = at * stride + field * rows + row
                    value = staged[k, pl.ds(first, size, stride=stride), :]
                    value = value + 1.0 if field == 0 else value * 1.5
                    slot = field * (rows // 2) + row % (rows // 2)
                    out[slot, :, k * LANES : (k + 1) * LANES] = value
        at += size


def spread(flat, chunks, rows, width, mib):
    half = FIELDS * (rows // 2)
    halves = width // LANES
    total = sum(size for _, size in chunks)
    shapes = [jax.ShapeDtypeStruct((half, size, width), F32) for _, size in chunks for _ in (0, 1)]
    out = pl.pallas_call(
        functools.partial(spread_body, chunks=chunks, rows=rows),
        in_specs=[pl.BlockSpec(memory_space=pl.ANY)],
        out_specs=[pl.BlockSpec(memory_space=pltpu.VMEM)] * len(shapes),
        out_shape=shapes,
        scratch_shapes=[
            pltpu.VMEM((halves, total * FIELDS * rows, LANES), F32),
            pltpu.SemaphoreType.DMA((halves * len(chunks),)),
        ],
        compiler_params=params(mib),
        name="spread",
    )(flat)
    return [(out[2 * i], out[2 * i + 1]) for i in range(len(chunks))]


def shifted(x, width):
    return pltpu.roll(x, width - 1, 1), pltpu.roll(x, 1, 1)


def prepared(h, u, v):
    vm, vp = 1.0 - v, 1.0 + v
    return h, u, v, vm, vp, h * vm, h * vp


def advance_row(south, middle, north, width, last):
    hs, us, vs, _, _, _, flow_s = south
    h, u, v, vm, vp, _, _ = middle
    hn, un, vn, _, _, flow_n, _ = north
    he, hw = shifted(h, width)
    ue, uw = shifted(u, width)
    ve, vw = shifted(v, width)
    um, up = 1.0 - u, 1.0 + u
    h_sum = (he * (1.0 - ue) + hw * (1.0 + uw)) + (flow_n + flow_s)
    u_sum = (ue * um + uw * up) + (un * vm + us * vp)
    v_sum = (ve * um + vw * up) + (vn * vm + vs * vp)
    h_new = 0.6 * h + 0.1 * h_sum
    u_new = (0.6 * u + 0.15 * v) + 0.1 * u_sum - 0.225 * (he - hw)
    v_new = (0.6 * v - 0.15 * u) + 0.1 * v_sum - 0.225 * (hn - hs)
    if last:
        return h_new - 1.0, u_new * (2.0 / 3.0), v_new * (2.0 / 3.0)
    return h_new, u_new, v_new


def owned_runs(units, parts, rows):
    each = units // parts
    whole = each // rows * rows
    runs = [(whole, 0), (each - whole, parts * whole)]
    return [run for run in runs if run[0]]


def forecast_body(
    me_ref, prev_ref, top_ref, bot_ref, next_ref, onehot_ref, *refs, begin, rows, size, block,
    width, parts, obs
):
    work, kept, onehot, sem, state_sems = refs[-5:]
    state_ref, *sends = refs[-6 - parts : -5]
    half = rows // 2
    total = rows + 2 * STEPS
    sources = (prev_ref, top_ref, bot_ref, next_ref)
    halves = width // LANES
    units = FIELDS * rows * halves
    each = units // parts
    place = pl.program_id(0)
    fetch = pltpu.make_async_copy(onehot_ref, onehot, sem)

    @pl.when(place == 0)
    def _():
        fetch.start()

    def group(index, carry):
        members = pl.ds(pl.multiple_of(index * 8, 8), 8)
        kept_members = pl.ds(pl.multiple_of(place * block + index * 8, 8), 8)

        def first(row):
            ref = sources[row // half]
            return prepared(*(ref[f * half + row % half, members, :] for f in range(FIELDS)))

        def later(step):
            return lambda row: prepared(
                *(work[(step - 1) % 2, f * total + row] for f in range(FIELDS))
            )

        for step in range(STEPS):
            load = first if step == 0 else later(step)
            last = step == STEPS - 1
            lo, hi = step + 1, total - 1 - step
            window = [load(lo - 1), load(lo)]
            for row in range(lo, hi):
                window.append(load(row + 1))
                new = advance_row(window[0], window[1], window[2], width, last)
                window.pop(0)
                for f in range(FIELDS):
                    if last:
                        for k in range(halves):
                            unit = (f * halves + k) * rows + row - STEPS
                            value = new[f][:, k * LANES : (k + 1) * LANES]
                            kept[unit, kept_members, :] = value
                    else:
                        work[step % 2, f * total + row] = new[f]
        return carry

    lax.fori_loop(0, block // 8, group, 0)

    def keep(index):
        source = pl.ds(pl.multiple_of(index * block, 8), block)
        target = pl.ds(pl.multiple_of(begin + index * block, 8), block)
        return pltpu.make_async_copy(
            kept.at[:, source, :], state_ref.at[:, target, :], state_sems.at[index]
        )

    keep(place).start()

    @pl.when(place == pl.num_programs(0) - 1)
    def _():
        fetch.wait()
        observed = jnp.zeros((size, obs), F32)
        for f in range(FIELDS):
            for row in range(rows):
                x = jnp.concatenate(
                    [kept[(f * halves + k) * rows + row] for k in range(halves)], axis=1
                )
                high = x.astype(BF16)
                rest = x - high.astype(F32)
                mid = rest.astype(BF16)
                low = (rest - mid.astype(F32)).astype(BF16)
                stacked = jnp.concatenate([high, mid, low], axis=0)
                part = dot(stacked, onehot[f * rows + row])
                observed = observed + ((part[:size] + part[size : 2 * size]) + part[2 * size :])
        me = me_ref[0]
        for p in range(parts):
            slot = 0
            for count, base in owned_runs(units, parts, rows):
                for j in range(count):
                    sends[p][slot] = kept[base + (me ^ p) * count + j]
                    slot += 1
            for k in range(obs // LANES):
                sends[p][each + k] = observed[:, k * LANES : (k + 1) * LANES]
        for index in range(size // block):
            keep(index).wait()


def forecast_chunk(
    me, prev, top, bot, nxt, onehot, state, begin, size, members, rows, width, parts, obs
):
    units = FIELDS * rows * (width // LANES)
    each = units // parts + obs // LANES
    half = FIELDS * (rows // 2)
    block = 16 if size % 16 == 0 else 8
    extra = [] if state is None else [state]
    return pl.pallas_call(
        functools.partial(
            forecast_body, begin=begin, rows=rows, size=size, block=block, width=width,
            parts=parts, obs=obs
        ),
        grid=(size // block,),
        in_specs=[pl.BlockSpec(memory_space=pltpu.SMEM)]
        + [pl.BlockSpec((half, block, width), lambda i: (0, i, 0))] * 4
        + [pl.BlockSpec(memory_space=pl.ANY)] * (1 + len(extra)),
        out_specs=[pl.BlockSpec(memory_space=pl.ANY)]
        + [pl.BlockSpec((each, size, LANES), lambda i: (0, 0, 0))] * parts,
        out_shape=[jax.ShapeDtypeStruct((units, SPARE * members, LANES), F32)]
        + [jax.ShapeDtypeStruct((each, size, LANES), F32)] * parts,
        scratch_shapes=[
            pltpu.VMEM((2, FIELDS * (rows + 2 * STEPS), 8, width), F32),
            pltpu.VMEM((units, size, LANES), F32),
            pltpu.VMEM(onehot.shape, BF16),
            pltpu.SemaphoreType.DMA,
            pltpu.SemaphoreType.DMA((size // block,)),
        ],
        compiler_params=params(),
        cost_estimate=pl.CostEstimate(flops=50_000_000, bytes_accessed=8_000_000, transcendentals=0),
        input_output_aliases={6: 0} if extra else {},
        name="forecast",
    )(me, prev, top, bot, nxt, onehot, *extra)


def joined_observed(blocks, each, obs):
    return jnp.concatenate(
        [
            jnp.concatenate([ref[each + k] for k in range(obs // LANES)], axis=1)
            for ref in blocks
        ],
        axis=0,
    )


def centred_products(blocks, each, obs, emit):
    scale = 1.0 / sum(ref.shape[1] for ref in blocks)
    y = joined_observed(blocks, each, obs)
    y_mean = jnp.sum(y, axis=0, keepdims=True) * scale
    perturbed = y - y_mean
    squares = jnp.sum(perturbed * perturbed, axis=0, keepdims=True)
    high, low = split2(perturbed.T)
    both = jnp.concatenate([high, low], axis=0)
    count = each + obs // LANES
    step = 2 if count % 2 == 0 else 1
    for unit in range(0, count, step):
        x = jnp.concatenate(
            [jnp.concatenate([ref[unit + k] for ref in blocks], axis=0) for k in range(step)],
            axis=1,
        )
        x_mean = jnp.sum(x, axis=0, keepdims=True) * scale
        d_high, d_low = split2(x - x_mean)
        part = dot(both, d_high)
        product = (part[:obs] + part[obs:]) + dot(high, d_low)
        for k in range(step):
            lanes = slice(k * LANES, (k + 1) * LANES)
            emit(unit + k, product[:, lanes], x_mean[:, lanes])
    return y_mean, squares


def early_body(*refs, count, each, obs):
    blocks = refs[:count]
    product_ref, mean_ref, y_ref = refs[count:]

    def emit(unit, product, mean):
        product_ref[unit] = product
        mean_ref[unit : unit + 1, :] = mean

    y_mean, squares = centred_products(blocks, each, obs, emit)
    y_ref[0:1, :] = y_mean
    y_ref[1:2, :] = squares


def early_covariance(blocks, each, obs):
    vmem = pl.BlockSpec(memory_space=pltpu.VMEM)
    return pl.pallas_call(
        functools.partial(early_body, count=len(blocks), each=each, obs=obs),
        in_specs=[vmem] * len(blocks),
        out_specs=[vmem] * 3,
        out_shape=[
            jax.ShapeDtypeStruct((each + obs // LANES, obs, LANES), F32),
            jax.ShapeDtypeStruct((each + obs // LANES, LANES), F32),
            jax.ShapeDtypeStruct((2, obs), F32),
        ],
        compiler_params=params(),
        cost_estimate=pl.CostEstimate(
            flops=10_000_000, bytes_accessed=8_000_000, transcendentals=0
        ),
        name="early",
    )(*blocks)


def late_body(
    target_ref, variance_ref, product_ref, mean_ref, y_ref, *refs, count, each, obs, first, before
):
    blocks = refs[:count]
    first_ref, second_ref, sums_ref, y_mean_ref, gram_ref = refs[count:]
    after = sum(ref.shape[1] for ref in blocks)
    total = before + after
    share = after / total
    cross = before * share
    y_late = jnp.sum(joined_observed(blocks, each, obs), axis=0, keepdims=True) * (1.0 / after)
    y_shift = y_late - y_ref[0:1, :]
    column = jnp.broadcast_to(cross * y_shift, (8, obs)).T[:, 0:1]

    def emit(unit, product, mean):
        old = mean_ref[unit : unit + 1, :]
        shift = mean - old
        value = product_ref[unit] + product + column * shift
        if unit >= each:
            gram_ref[:, (unit - each) * LANES : (unit - each + 1) * LANES] = value
            return
        out, at = (first_ref, unit) if unit < first else (second_ref, unit - first)
        out[at * obs : (at + 1) * obs, :] = value
        tail = (first if unit < first else each - first) * obs + at
        out[tail : tail + 1, :] = old + share * shift

    _, squares = centred_products(blocks, each, obs, emit)
    y_mean = y_ref[0:1, :] + share * y_shift
    misfit = target_ref[...] - y_mean
    spread = (y_ref[1:2, :] + squares + cross * y_shift * y_shift) / (total - 1)
    sums_ref[0:1, :] = misfit * misfit
    sums_ref[1:2, :] = spread + variance_ref[...]
    y_mean_ref[...] = jnp.broadcast_to(y_mean, y_mean_ref.shape)


def padded(count):
    return -(-count // 8) * 8


def late_covariance(target, variance, early, blocks, each, obs, before):
    vmem = pl.BlockSpec(memory_space=pltpu.VMEM)
    first = (each + 1) // 2
    second = each - first
    return pl.pallas_call(
        functools.partial(
            late_body, count=len(blocks), each=each, obs=obs, first=first, before=before
        ),
        in_specs=[vmem] * (5 + len(blocks)),
        out_specs=[vmem] * 5,
        out_shape=[
            jax.ShapeDtypeStruct((first * obs + padded(first), LANES), F32),
            jax.ShapeDtypeStruct((second * obs + padded(second), LANES), F32),
            jax.ShapeDtypeStruct((2, obs), F32),
            jax.ShapeDtypeStruct((8, obs), F32),
            jax.ShapeDtypeStruct((obs, obs), F32),
        ],
        compiler_params=params(),
        cost_estimate=pl.CostEstimate(
            flops=10_000_000, bytes_accessed=8_000_000, transcendentals=0
        ),
        name="late",
    )(target, variance, *early, *blocks)


def weights_body(
    sums_ref, target_ref, variance_ref, mean_ref, gram_ref, *refs, count, obs, total
):
    tails = obs // LANES
    blocks = [refs[i * tails : (i + 1) * tails] for i in range(count)]
    weights_ref, scale_ref = refs[count * tails :]

    def observed(slabs):
        return jnp.concatenate([slab[0] for slab in slabs], axis=1)

    y_mean = mean_ref[0:1, :]
    inflation = sums_ref[0:1, 0:1] / sums_ref[0:1, 1:2]
    factor = inflation / (total - 1)
    variance = variance_ref[...]
    weighted = (target_ref[...] - y_mean) / variance
    gram = gram_ref[...]
    g_row = jnp.sqrt(factor / variance)
    eye = (
        lax.broadcasted_iota(jnp.int32, (obs, obs), 0)
        == lax.broadcasted_iota(jnp.int32, (obs, obs), 1)
    ).astype(F32)
    g_col = jnp.sum(eye * g_row, axis=1, keepdims=True)
    kernel = gram * g_row * g_col
    norm = jnp.sum(jnp.sum(kernel * kernel, axis=1, keepdims=True), axis=0, keepdims=True)
    bound = 2.0 + jnp.sqrt(norm)
    slope = 2.0 / (bound - 1.0)
    angles = [(j + 0.5) * (math.pi / (DEGREE + 1)) for j in range(DEGREE + 1)]
    values = [
        lax.rsqrt(0.5 * (bound + 1.0) + 0.5 * (bound - 1.0) * math.cos(angle))
        for angle in angles
    ]
    coeffs = []
    for k in range(DEGREE + 1):
        term = sum(math.cos(k * angle) * value for angle, value in zip(angles, values))
        coeffs.append((2.0 if k else 1.0) / (DEGREE + 1) * term)
    base = coeffs[0] - coeffs[1]
    shifted_kernel = slope * kernel - eye
    before = jnp.zeros((obs, obs), F32)
    current = slope * eye
    summed = coeffs[1] * current
    for k in range(1, DEGREE):
        sign = -1.0 if k % 2 else 1.0
        if k == 1:
            product = slope * shifted_kernel
        else:
            product = dot_full(shifted_kernel, current)
        following = 2.0 * product - before + (2.0 * sign) * slope * eye
        summed = summed + coeffs[k + 1] * following
        base = base - sign * coeffs[k + 1]
        before, current = current, following
    middle = summed * g_row * g_col
    row = jnp.broadcast_to(weighted, (8, obs))
    for _ in range(2):
        row = base * row + dot_full(dot_full(row, gram), middle)
    row = factor * row[0:1, :]
    root = jnp.sqrt(inflation)
    own = jnp.concatenate([observed(block) for block in blocks], axis=0) - y_mean
    weights_ref[...] = dot_full(own, root * middle) + row
    scale_ref[...] = jnp.broadcast_to(root * base, scale_ref.shape)


def make_weights(sums, target, variance, mean, gram, blocks, each, obs, parts):
    vmem = pl.BlockSpec(memory_space=pltpu.VMEM)
    own = sum(block.shape[1] for block in blocks)
    total = parts * own
    tails = obs // LANES
    slabs, specs = [], []
    for block in blocks:
        for k in range(tails):
            slabs.append(block)
            specs.append(pl.BlockSpec((1, block.shape[1], LANES), lambda i, k=k: (each + k, 0, 0)))
    return pl.pallas_call(
        functools.partial(weights_body, count=len(blocks), obs=obs, total=total),
        grid=(1,),
        in_specs=[vmem] * 5 + specs,
        out_specs=[vmem] * 2,
        out_shape=[
            jax.ShapeDtypeStruct((own, obs), F32),
            jax.ShapeDtypeStruct((8, LANES), F32),
        ],
        compiler_params=params(),
        cost_estimate=pl.CostEstimate(
            flops=10_000_000, bytes_accessed=2_000_000, transcendentals=0
        ),
        name="weights",
    )(sums, target, variance, mean, gram, *slabs)


def segments(begin, end, units, parts, rows):
    found, slot = [], 0
    for count, base in owned_runs(units, parts, rows):
        lo, hi = max(begin, slot), min(end, slot + count)
        if lo < hi:
            found.append((lo - begin, hi - lo, base + lo - slot, count))
        slot += count
    return found


def update_body(
    tiles_ref, owner_ref, scale_ref, weights_ref, *refs, chunks, bounds, units, parts, rows, obs
):
    states = refs[:chunks]
    pieces = refs[chunks : chunks + len(bounds)]
    out_ref, gathered, means, split_w, turned = refs[-5:]
    members = weights_ref.shape[0]

    @pl.when(pl.program_id(0) == 0)
    def _():
        high, low = split2(weights_ref[...])
        split_w[:members] = high
        split_w[members:] = low
        for index, (begin, end) in enumerate(bounds):
            owner = owner_ref[index]
            piece = pieces[index]
            tail = (end - begin) * obs
            for slot, count, base, stride in segments(begin, end, units, parts, rows):
                for j in range(slot, slot + count):
                    unit = base + owner * stride + j - slot
                    gathered[unit] = piece[j * obs : (j + 1) * obs, :]
                    means[unit] = jnp.broadcast_to(
                        piece[tail + j : tail + j + 1, :], (8, LANES)
                    )

    tile = tiles_ref[pl.program_id(0)]
    scale = scale_ref[0:1, :]
    high = split_w[:members]
    both = split_w[...]
    for row in range(0, rows, 2):
        unit = tile * rows + row
        c = [gathered[unit + k] for k in range(2)]
        c_high, c_low = split2(jnp.concatenate(c, axis=1))
        part = dot(both, c_high)
        product = (part[:members] + part[members:]) + dot(high, c_low)
        for k in range(2):
            x = jnp.concatenate([ref[0, row + k] for ref in states], axis=0)
            turned[pl.ds(row + k, members, stride=rows), :] = (
                product[:, k * LANES : (k + 1) * LANES]
                + scale * x
                + (1.0 - scale) * means[unit + k, 0:1, :]
            )
    out_ref[:, 0, :, :] = turned[...].reshape(members, rows, LANES)


def update(tiles, scale, weights, states, pieces, owners, bounds, rows, width, obs, parts, into):
    members = weights.shape[0]
    halves = width // LANES
    units = FIELDS * rows * halves
    views = [s.reshape(FIELDS * halves, rows, s.shape[1], LANES) for s in states]
    vmem = pl.BlockSpec(memory_space=pltpu.VMEM)
    extra = [] if into is None else [into]
    body = functools.partial(
        update_body, chunks=len(states), bounds=bounds, units=units, parts=parts, rows=rows, obs=obs
    )
    operands = [scale, weights, *views, *pieces, *extra]
    return pl.pallas_call(
        body,
        grid_spec=pltpu.PrefetchScalarGridSpec(
            num_scalar_prefetch=2,
            grid=(tiles.shape[0],),
            in_specs=[
                pl.BlockSpec(scale.shape, lambda i, t, o: (0, 0)),
                pl.BlockSpec(weights.shape, lambda i, t, o: (0, 0)),
            ]
            + [
                pl.BlockSpec((1, rows, members, LANES), lambda i, t, o: (t[i], 0, 0, 0))
                for v in views
            ]
            + [pl.BlockSpec(piece.shape, lambda i, t, o: (0, 0)) for piece in pieces]
            + [pl.BlockSpec(memory_space=pl.ANY)] * len(extra),
            out_specs=pl.BlockSpec(
                (members, 1, rows, LANES), lambda i, t, o: (0, t[i] // halves, 0, t[i] % halves)
            ),
            scratch_shapes=[
                pltpu.VMEM((units, obs, LANES), F32),
                pltpu.VMEM((units, 8, LANES), F32),
                pltpu.VMEM((2 * members, obs), BF16),
                pltpu.VMEM((members * rows, LANES), F32),
            ],
        ),
        out_shape=jax.ShapeDtypeStruct((members, FIELDS, rows, width), F32),
        input_output_aliases={} if into is None else {2 + len(operands) - 1: 0},
        compiler_params=params(),
        cost_estimate=pl.CostEstimate(
            flops=10_000_000, bytes_accessed=20_000_000, transcendentals=0
        ),
        name="update" if into is None else "finish",
    )(tiles, owners, *operands)


def chunk_plan(members):
    unit = members // 16
    if unit % 8:
        size = members // CHUNKS
        return [(size * i, size) for i in range(CHUNKS)]
    shares = [(0, 2), (2, 3), (5, 3), (8, 3), (11, 3), (14, 2)]
    return [(unit * begin, unit * size) for begin, size in shares]


def spread_groups(count):
    return [(0, AHEAD - 1), (AHEAD - 1, AHEAD), (AHEAD, count)]


def step(ensemble, obs_cells, region_tile, obs_values, obs_error):
    members, _, rows, width = ensemble.shape
    parts = lax.axis_size("mem")
    tiles = lax.axis_size("tile")
    obs = obs_cells.shape[1]
    halves = width // LANES
    units = FIELDS * rows * halves
    each = units // parts
    plan = chunk_plan(members)
    order = sorted(range(len(plan)), key=lambda chunk: plan[chunk])
    up = [(i, (i + 1) % tiles) for i in range(tiles)]
    down = [((i + 1) % tiles, i) for i in range(tiles)]

    def swap(x, p):
        return lax.ppermute(x, "mem", [(i, i ^ p) for i in range(parts)])

    me = jnp.reshape(lax.axis_index("mem"), (1,)).astype(jnp.int32)
    flat = ensemble.reshape(members * FIELDS * rows, width)

    chosen = (region_tile == lax.axis_index("tile"))[:, None]
    obs_index = jnp.sum(jnp.where(chosen, obs_cells, 0), axis=0)
    target = jnp.sum(jnp.where(chosen, obs_values, 0.0), axis=0, keepdims=True)
    variance = jnp.sum(jnp.where(chosen, obs_error, 0.0), axis=0, keepdims=True)
    cells = lax.broadcasted_iota(jnp.int32, (FIELDS * rows, width, obs), 0) * width
    cells = cells + lax.broadcasted_iota(jnp.int32, (FIELDS * rows, width, obs), 1)
    onehot = (cells == obs_index[None, None, :]).astype(BF16)

    pairs = []
    for group, (begin, end) in enumerate(spread_groups(len(plan))):
        mib = REST_VMEM_MIB if group == 2 else SPREAD_VMEM_MIB
        pairs += spread(flat, plan[begin:end], rows, width, mib)

    def halo(chunk):
        top, bot = pairs[chunk]
        prev = lax.ppermute(bot, "tile", up)
        return prev, top, bot, lax.ppermute(top, "tile", down)

    blocks, mine, state = [], [], None
    for chunk, (begin, size) in enumerate(plan):
        prev, top, bot, nxt = halo(chunk)
        state, *sends = forecast_chunk(
            me, prev, top, bot, nxt, onehot, state, begin, size, members, rows, width, parts, obs
        )
        mine.append(sends[0])
        blocks.append(sends[0])
        for p in reversed(range(1, parts)):
            blocks.append(swap(sends[p], p))

    late = len(blocks) - parts
    early = early_covariance(blocks[:late], each, obs)
    c_first, c_second, sums, y_mean, gram = late_covariance(
        target, variance, early, blocks[late:], each, obs, parts * (members - plan[-1][1])
    )
    first = (each + 1) // 2
    bounds = [(0, first), (first, each)]
    sums = lax.psum(jnp.sum(sums, axis=1)[None, :], "tile")
    weights, scale = make_weights(
        sums, target, variance, y_mean, gram, [mine[chunk] for chunk in order], each, obs, parts
    )
    args = (scale, weights, [state])
    sizes_of = (rows, width, obs, parts)
    if parts == 4 and each == rows + rows // 2:
        x_first, y_second = swap(c_first, 1), swap(c_second, 2)
        x_second, y_first = swap(c_second, 1), swap(c_first, 2)
        far_first, far_second = swap(x_first, 2), swap(y_second, 1)
        own, x, y, far = me, me ^ 1, me ^ 2, me ^ 3
        done = update(
            jnp.concatenate([own, x, y, parts + own // 2]),
            *args,
            [c_first, c_second, x_first, x_second, y_first, y_second],
            jnp.concatenate([own, own, x, x, y, y]),
            bounds * 3,
            *sizes_of,
            None,
        )
        return update(
            jnp.concatenate([far, parts + far // 2]),
            *args,
            [far_first, far_second, y_second],
            jnp.concatenate([far, far, y]),
            bounds + bounds[1:],
            *sizes_of,
            done,
        )
    pieces, owners = [], []
    for p in range(parts):
        for piece in (c_first, c_second):
            pieces.append(swap(piece, p) if p else piece)
            owners.append(me ^ p)
    return update(
        jnp.arange(FIELDS * halves, dtype=jnp.int32),
        *args,
        pieces,
        jnp.concatenate(owners),
        bounds * parts,
        *sizes_of,
        None,
    )


def solution(mesh):
    in_specs = (P("mem", None, "tile", None), P(), P(), P(), P())
    out_specs = P("mem", None, "tile", None)
    return jax.shard_map(step, mesh=mesh, in_specs=in_specs, out_specs=out_specs, check_vma=False)
```
